32 devices in a mesh: section: 4 (over y, core), dp: 2 (over x), tensor: 4 (over z).
Axes of the slice: x: 2, y: 2, z: 4, core: 2. Of those that a mesh axis runs over, the one named last changes fastest.
Arguments:
- shadow_weight_copy: bfloat16 [4, 4096, 4096], P('section', None, 'tensor'), may hold values from -6 to 6
- newest_weight_version: bfloat16 [4, 4096, 4096], P('section', 'dp', 'tensor'), may hold values from -6 to 6
- momentum: bfloat16 [4, 4096, 4096], P('section', 'dp', 'tensor'), may hold values from -3 to 3
- pending_section_input: bfloat16 [2, 4, 64, 4096], P('dp', 'section', None, 'tensor'), may hold values from -16 to 16
- incoming_micro_input: bfloat16 [2, 3, 64, 4096], P('dp', None, None, 'tensor'), may hold values from -16 to 16
- pending_output_gradient: bfloat16 [2, 4, 64, 4096], P('dp', 'section', None, 'tensor'), may hold values from -16 to 16
- loss_gradient_rows: bfloat16 [2, 3, 64, 4096], P('dp', None, None, 'tensor'), may hold values from -16 to 16
- stashed: bfloat16 [2, 4, 4, 64, 4096], P('dp', 'section', None, None, 'tensor'), may hold values from -16 to 16
Outputs:
- forward_out: bfloat16 [2, 4, 4, 64, 4096], P('dp', 'section', None, None, 'tensor')
- backward_out: bfloat16 [2, 4, 4, 64, 4096], P('dp', 'section', None, None, 'tensor')
- w_next: bfloat16 [4, 4096, 4096], P('section', 'dp', 'tensor')
- m_next: bfloat16 [4, 4096, 4096], P('section', 'dp', 'tensor')
The draws below stay inside these ranges and needn't reach their ends.
All inputs are finite; a program needn't handle non-finite values.
Results may differ from the reference program's by a relative error of at most 0.025.
Values may be sent and summed in bfloat16 or wider, within the bound.
No kernel may reach another device: no remote copies, remote signals or barrier semaphores. Data moves between devices by JAX's collectives and lax.ppermute only.
A program may use at most 128 MiB of HBM per device.

```python
import math
import jax
import jax.numpy as jnp
from jax import lax

D = 4096
ROWS = 64
TICKS = 4
SECTIONS = 4
REPLICAS = 2
N_TENSOR = 4


def feature_field(key, dimensions):
    extent = dimensions[-1]
    random_part = jax.random.normal(jax.random.fold_in(key, 1), dimensions, jnp.float32)
    growth = jnp.exp(jnp.log(3.0) * jnp.arange(extent, dtype=jnp.float32) / (extent - 1))
    result_field = random_part * growth / jnp.sqrt(jnp.mean(growth * growth))
    return jnp.clip(result_field, -16.0, 16.0).astype(jnp.bfloat16)


def draw_pending_section_input(key, part):
    return feature_field(jax.random.fold_in(key, 101), (REPLICAS, SECTIONS, ROWS, D))


def draw_incoming_micro_input(key, part):
    return feature_field(jax.random.fold_in(key, 102), (REPLICAS, TICKS - 1, ROWS, D))


def draw_pending_output_gradient(key, part):
    return feature_field(jax.random.fold_in(key, 103), (REPLICAS, SECTIONS, ROWS, D))


def draw_loss_gradient_rows(key, part):
    return feature_field(jax.random.fold_in(key, 104), (REPLICAS, TICKS - 1, ROWS, D))


def draw_stashed(key, part):
    return feature_field(jax.random.fold_in(key, 105), (REPLICAS, SECTIONS, TICKS, ROWS, D))


def block_scale(rng, dims, cuts, least, largest):
    gain, own = 1.0, jax.random.fold_in(rng, 6)
    for position, shards_of in cuts:
        steps = jnp.exp(jax.random.uniform(jax.random.fold_in(own, position), (shards_of,), jnp.float32, least / len(cuts), largest / len(cuts)))
        gain = gain * jnp.repeat(steps, dims[position] // shards_of).reshape([-1 if axis == position else 1 for axis in range(len(dims))])
    return gain


def scatter_about(own_key, shape, spread, bound, split=(), kind=jnp.bfloat16):
    values = spread * jax.random.normal(own_key, shape, jnp.float32)
    if split:
        values = values * block_scale(own_key, shape, split, -0.22, 0.18)
    return jnp.clip(values, -bound, bound).astype(kind)


def setup_inputs(seed: int = 0) -> dict:
    streams_of = jax.random.split(jax.random.key(seed), 9)
    shadow_weight_copy = scatter_about(streams_of[0], (SECTIONS, D, D), 1.0, 6.0, ((0, 4), (2, 4)))
    newest_weight_version = scatter_about(streams_of[1], (SECTIONS, D, D), 1.0, 6.0, ((0, 4), (1, 2), (2, 4)))
    momentum = scatter_about(streams_of[2], (SECTIONS, D, D), 0.5, 3.0, ((0, 4), (1, 2), (2, 4)))
    pending_section_input = draw_pending_section_input(jax.random.fold_in(streams_of[8], 71), 0)
    incoming_micro_input = draw_incoming_micro_input(jax.random.fold_in(streams_of[8], 71), 0)
    pending_output_gradient = draw_pending_output_gradient(jax.random.fold_in(streams_of[8], 71), 0)
    loss_gradient_rows = draw_loss_gradient_rows(jax.random.fold_in(streams_of[8], 71), 0)
    stashed = draw_stashed(jax.random.fold_in(streams_of[8], 71), 0)
    return {"shadow_weight_copy": shadow_weight_copy, "newest_weight_version": newest_weight_version, "momentum": momentum, "pending_section_input": pending_section_input, "incoming_micro_input": incoming_micro_input, "pending_output_gradient": pending_output_gradient, "loss_gradient_rows": loss_gradient_rows, "stashed": stashed}


EPSILON = 1e-06
MOMENTUM_RATE = 0.9
LEARNING_RATE = 0.05

def normalized(values):
    factor = lax.rsqrt(lax.optimization_barrier(jnp.mean(values * values, axis=-1, keepdims=True)) + EPSILON)
    return (values * factor, factor)

def rounded(values):
    return lax.optimization_barrier(values.astype(jnp.bfloat16)).astype(jnp.float32)

def section_tick(operands):
    current_input, kept_in, grad_in, weight = operands
    extent = weight.shape[0]
    root_width = math.sqrt(extent)
    weight_wide = weight.astype(jnp.float32)
    x_wide = current_input.astype(jnp.float32)
    x_hat, unused = normalized(x_wide)
    branch = jnp.einsum('prd,de->pre', rounded(x_hat), weight_wide) / root_width
    section_out = (x_wide + branch).astype(jnp.bfloat16)
    kept_hat, kept_factor = normalized(kept_in.astype(jnp.float32))
    grad_wide = grad_in.astype(jnp.float32)
    replicas = grad_in.shape[0]
    row_count = grad_in.shape[1]
    shard_cols = extent // N_TENSOR
    grad_pieces = grad_wide.reshape(replicas, row_count, N_TENSOR, shard_cols)
    weight_pieces = weight_wide.reshape(extent, N_TENSOR, shard_cols)
    partial_value = jnp.einsum('prje,dje->pjrd', grad_pieces, weight_pieces) / root_width
    branch_grad = lax.optimization_barrier(jnp.sum(rounded(partial_value), axis=1))
    inner_dot = lax.optimization_barrier(jnp.mean(branch_grad * kept_hat, axis=-1, keepdims=True))
    input_grad = (grad_wide + (branch_grad - kept_hat * inner_dot) * kept_factor).astype(jnp.bfloat16)
    return (section_out, input_grad, kept_hat.astype(jnp.bfloat16))

def section_update(operands):
    kept_rows, grad_rows, latest, moment = operands
    extent = latest.shape[0]
    replica_terms = jnp.einsum('pkrd,pkre->pde', kept_rows.astype(jnp.float32), grad_rows.astype(jnp.float32)) / math.sqrt(extent)
    summed = lax.optimization_barrier(jnp.sum(rounded(replica_terms), axis=0))
    velocity = MOMENTUM_RATE * moment.astype(jnp.float32) + summed
    new_weight = (latest.astype(jnp.float32) - LEARNING_RATE * velocity).astype(jnp.bfloat16)
    return (new_weight, velocity.astype(jnp.bfloat16))

def reference(shadow_weight_copy, newest_weight_version, momentum, pending_section_input, incoming_micro_input, pending_output_gradient, loss_gradient_rows, stashed):
    tick_count = stashed.shape[2]
    current_input = pending_section_input
    current_gradient = pending_output_gradient
    forward_list = []
    backward_list = []
    kept_list = []
    grad_list = []
    for tick_index in range(tick_count):
        if tick_index > 0:
            current_input = jnp.concatenate([incoming_micro_input[:, tick_index - 1][:, None], forward_list[-1][:, :-1]], axis=1)
            current_gradient = jnp.concatenate([backward_list[-1][:, 1:], loss_gradient_rows[:, tick_index - 1][:, None]], axis=1)
        operands = (jnp.moveaxis(current_input, 1, 0), jnp.moveaxis(stashed[:, :, tick_index], 1, 0), jnp.moveaxis(current_gradient, 1, 0), shadow_weight_copy)
        section_out, input_grad, kept_norm = lax.map(section_tick, operands)
        forward_list.append(jnp.moveaxis(section_out, 0, 1))
        backward_list.append(jnp.moveaxis(input_grad, 0, 1))
        kept_list.append(jnp.moveaxis(kept_norm, 0, 1))
        grad_list.append(current_gradient)
    forward_out = jnp.stack(forward_list, axis=2)
    backward_out = jnp.stack(backward_list, axis=2)
    kept_all = jnp.stack(kept_list, axis=2)
    grad_all = jnp.stack(grad_list, axis=2)
    w_next, m_next = lax.map(section_update, (jnp.moveaxis(kept_all, 1, 0), jnp.moveaxis(grad_all, 1, 0), newest_weight_version, momentum))
    return (forward_out, backward_out, w_next, m_next)
```

```python
import functools
import math

import jax
import jax.numpy as jnp
from jax import lax
from jax.experimental import pallas as pl
from jax.experimental.pallas import tpu as pltpu
from jax.sharding import PartitionSpec as P

EPSILON = 1e-06
MOMENTUM_RATE = 0.9
LEARNING_RATE = 0.05
LANES = 128
MIB = 1 << 20

BF16 = jnp.bfloat16
F32 = jnp.float32


def cyclic(block, distance):
    count = lax.axis_size("tensor")
    return lax.ppermute(block, "tensor", [(i, (i + distance) % count) for i in range(count)])


def gathered(block):
    return [block] + [cyclic(block, d) for d in range(1, lax.axis_size("tensor"))]


def gathered_from_below(block):
    sections, count = lax.axis_size("section"), lax.axis_size("tensor")
    result = []
    for d in range(count):
        route = [
            (s * count + t, ((s + 1) % sections) * count + (t + d) % count)
            for s in range(sections)
            for t in range(count)
        ]
        result.append(lax.ppermute(block, ("section", "tensor"), route))
    return result


def from_above(block):
    sections = lax.axis_size("section")
    return lax.ppermute(block, "section", [(s, (s - 1) % sections) for s in range(sections)])


def dp_cyclic(block, distance):
    count = lax.axis_size("dp")
    return lax.ppermute(block, "dp", [(i, (i + distance) % count) for i in range(count)])


def rows_of(w_ref, index, size):
    return w_ref[pl.ds(pl.multiple_of(index * size, size), size), :]


def row_factor(blocks, extent):
    total = sum(jnp.sum(b * b, axis=-1, keepdims=True) for b in blocks)
    return lax.rsqrt(total / extent + EPSILON)


def forward_kernel(count, with_payload, where_ref, w_ref, *refs):
    blocks, rest = refs[:count], refs[count:]
    extent, size = w_ref.shape[0], w_ref.shape[0] // count
    me = where_ref[0]
    acc = None
    for d in range(count):
        term = jnp.dot(
            blocks[d][...],
            rows_of(w_ref, lax.rem(me - d + count, count), size),
            preferred_element_type=F32,
        )
        acc = term if acc is None else acc + term
    factor = row_factor([b[...].astype(F32) for b in blocks], extent)
    out = (blocks[0][...].astype(F32) + acc * (factor * (1.0 / math.sqrt(extent)))).astype(BF16)
    if with_payload:
        incoming_ref, out_ref, payload_ref = rest
        payload_ref[...] = jnp.where(where_ref[2] == 1, incoming_ref[...], out)
    else:
        (out_ref,) = rest
    out_ref[...] = out


def backward_kernel(count, replicas, where_ref, w_ref, grad_ref, *refs):
    kept = refs[:count]
    payloads = refs[count : 2 * count]
    factor_ref = refs[2 * count]
    hats = refs[2 * count + 1 :]
    extent, size = w_ref.shape[0], w_ref.shape[0] // count
    root = 1.0 / math.sqrt(extent)
    me, rank = where_ref[0], where_ref[3]
    wide = [b[...].astype(F32) for b in kept]
    factor = row_factor(wide, extent)
    factor_ref[...] = jnp.broadcast_to(factor, factor_ref.shape)
    grad = grad_ref[...]
    total = None
    for d in range(count):
        term = (
            lax.dot_general(
                grad,
                rows_of(w_ref, lax.rem(me + d, count), size),
                (((1,), (1,)), ((), ())),
                preferred_element_type=F32,
            )
            * root
        ).astype(BF16)
        payloads[d][:, :size] = term
        part = jnp.sum(term.astype(F32) * wide[(count - d) % count], axis=-1, keepdims=True)
        total = part if total is None else total + part
    total = total * factor
    high = total.astype(BF16)
    middle = (total - high.astype(F32)).astype(BF16)
    low = (total - high.astype(F32) - middle.astype(F32)).astype(BF16)
    lane = lax.broadcasted_iota(jnp.int32, (grad.shape[0], LANES), 1)
    tail = jnp.where(
        lane == 0,
        high.astype(F32),
        jnp.where(lane == 1, middle.astype(F32), jnp.where(lane == 2, low.astype(F32), 0.0)),
    ).astype(BF16)
    for d in range(count):
        payloads[d][:, size:] = tail
    hat = [(w * factor).astype(BF16) for w in wide]
    per = count // replicas
    for r in range(replicas):
        owner = lax.rem(rank + r, replicas)
        for k in range(per):
            distance = lax.rem(me - (owner * per + k) + count, count)
            chosen = hat[0]
            for d in range(1, count):
                chosen = jnp.where(distance == d, hat[d], chosen)
            hats[r][k] = chosen


def combine_kernel(count, with_payload, where_ref, grad_ref, kept_ref, factor_ref, *refs):
    parts, rest = refs[:count], refs[count:]
    size = grad_ref.shape[1]
    own = sum(p[:, :size].astype(F32) for p in parts)
    inner = sum(jnp.sum(p[:, size:].astype(F32), axis=-1, keepdims=True) for p in parts)
    inner = inner / (size * count)
    factor = factor_ref[:, :1]
    hat = kept_ref[...].astype(F32) * factor
    out = (grad_ref[...].astype(F32) + (own - hat * inner) * factor).astype(BF16)
    if with_payload:
        loss_ref, out_ref, payload_ref = rest
        payload_ref[...] = jnp.where(where_ref[1] == 1, loss_ref[...], out)
    else:
        (out_ref,) = rest
    out_ref[...] = out


def update_kernel(pieces, root, *refs):
    hats, grads = refs[:pieces], refs[pieces : 2 * pieces]
    w_ref, m_ref, w_out, m_out, hat_all, grad_all = refs[2 * pieces :]
    rows = grads[0].shape[0]

    @pl.when(pl.program_id(0) == 0)
    def _():
        for i in range(pieces):
            size = hats[i].shape[2]
            for k in range(hats[i].shape[0]):
                hat_all[i * rows : (i + 1) * rows, k * size : (k + 1) * size] = hats[i][k]
            grad_all[i * rows : (i + 1) * rows, :] = grads[i][...]

    tile = w_ref.shape[0]
    start = pl.multiple_of(pl.program_id(0) * tile, tile)
    summed = (
        lax.dot_general(
            hat_all[:, pl.ds(start, tile)],
            grad_all[...],
            (((0,), (0,)), ((), ())),
            preferred_element_type=F32,
        )
        * root
    )
    velocity = MOMENTUM_RATE * m_ref[...].astype(F32) + summed
    w_out[...] = (w_ref[...].astype(F32) - LEARNING_RATE * velocity).astype(BF16)
    m_out[...] = velocity.astype(BF16)


SMEM_SPEC = pl.BlockSpec(memory_space=pltpu.SMEM)
VMEM_SPEC = pl.BlockSpec(memory_space=pltpu.VMEM)


def cost(flops, moved):
    return pl.CostEstimate(flops=flops, bytes_accessed=moved, transcendentals=0)


def call(kernel, shapes, flops, limit, *operands):
    moved = sum(math.prod(o.shape) * o.dtype.itemsize for o in operands + tuple(shapes))
    return pl.pallas_call(
        kernel,
        out_shape=shapes,
        in_specs=[SMEM_SPEC] + [VMEM_SPEC] * (len(operands) - 1),
        out_specs=[VMEM_SPEC] * len(shapes),
        compiler_params=pltpu.CompilerParams(vmem_limit_bytes=limit),
        cost_estimate=cost(flops, moved),
    )(*operands)


def update(hats, grads, newest, momentum, root):
    rows, cols = newest.shape
    tile = min(256, hats[0].shape[2])
    pieces = len(hats)
    depth = pieces * grads[0].shape[0]
    whole = [pl.BlockSpec(h.shape, lambda i: (0, 0, 0)) for h in hats]
    whole += [pl.BlockSpec(g.shape, lambda i: (0, 0)) for g in grads]
    tiled = pl.BlockSpec((tile, cols), lambda i: (i, 0))
    shape = jax.ShapeDtypeStruct(newest.shape, BF16)
    return pl.pallas_call(
        functools.partial(update_kernel, pieces, root),
        grid=(rows // tile,),
        out_shape=[shape, shape],
        in_specs=whole + [tiled, tiled],
        out_specs=[tiled, tiled],
        scratch_shapes=[pltpu.VMEM((depth, rows), BF16), pltpu.VMEM((depth, cols), BF16)],
        compiler_params=pltpu.CompilerParams(vmem_limit_bytes=32 * MIB),
        cost_estimate=cost(2 * depth * rows * cols, 8 * rows * cols),
    )(*hats, *grads, newest, momentum)


def body(
    shadow_weight_copy,
    newest_weight_version,
    momentum,
    pending_section_input,
    incoming_micro_input,
    pending_output_gradient,
    loss_gradient_rows,
    stashed,
):
    weight = shadow_weight_copy[0]
    extent, size = weight.shape
    root = 1.0 / math.sqrt(extent)
    tick_count, rows = stashed.shape[2], stashed.shape[3]
    count, replicas = lax.axis_size("tensor"), lax.axis_size("dp")
    section = lax.axis_index("section")
    where = jnp.stack(
        [
            lax.axis_index("tensor"),
            (section == 0).astype(jnp.int32),
            (section == lax.axis_size("section") - 1).astype(jnp.int32),
            lax.axis_index("dp"),
        ]
    ).astype(jnp.int32)
    block = jax.ShapeDtypeStruct((rows, size), BF16)
    wide_block = jax.ShapeDtypeStruct((rows, size + LANES), BF16)
    factor_shape = jax.ShapeDtypeStruct((rows, LANES), F32)
    hat_shape = jax.ShapeDtypeStruct((count // replicas, rows, size), BF16)
    flops = 2 * rows * extent * size
    grad = pending_output_gradient[0, 0]
    x_blocks = gathered(pending_section_input[0, 0])
    forward_list, backward_list, hats, grads = [], [], [], []
    for t in range(tick_count):
        last = t == tick_count - 1
        kept = gathered(stashed[0, 0, t])
        outs = call(
            functools.partial(backward_kernel, count, replicas),
            [wide_block] * count + [factor_shape] + [hat_shape] * replicas,
            flops,
            24 * MIB,
            where,
            weight,
            grad,
            *kept,
        )
        payloads, factor, halves = outs[:count], outs[count], outs[count + 1 :]
        for r in range(replicas):
            hats.append(halves[r] if r == 0 else dp_cyclic(halves[r], r))
            grads.append(grad if r == 0 else dp_cyclic(grad, r))
        parts = [payloads[0]] + [cyclic(payloads[d], d) for d in range(1, count)]
        outs = call(
            functools.partial(forward_kernel, count, not last),
            [block] if last else [block, block],
            flops,
            24 * MIB,
            where,
            weight,
            *x_blocks,
            *([] if last else [incoming_micro_input[0, t]]),
        )
        forward_list.append(outs[0])
        if not last:
            x_blocks = gathered_from_below(outs[1])
        outs = call(
            functools.partial(combine_kernel, count, not last),
            [block] if last else [block, block],
            rows * size * 16,
            8 * MIB,
            where,
            grad,
            kept[0],
            factor,
            *parts,
            *([] if last else [loss_gradient_rows[0, t]]),
        )
        backward_list.append(outs[0])
        if not last:
            grad = from_above(outs[1])
    w_next, m_next = update(hats, grads, newest_weight_version[0], momentum[0], root)
    forward_out = jnp.stack(forward_list, axis=0)[None, None]
    backward_out = jnp.stack(backward_list, axis=0)[None, None]
    return (forward_out, backward_out, w_next[None], m_next[None])


def solution(mesh):
    return jax.shard_map(
        body,
        mesh=mesh,
        in_specs=(
            P("section", None, "tensor"),
            P("section", "dp", "tensor"),
            P("section", "dp", "tensor"),
            P("dp", "section", None, "tensor"),
            P("dp", None, None, "tensor"),
            P("dp", "section", None, "tensor"),
            P("dp", None, None, "tensor"),
            P("dp", "section", None, None, "tensor"),
        ),
        out_specs=(
            P("dp", "section", None, None, "tensor"),
            P("dp", "section", None, None, "tensor"),
            P("section", "dp", "tensor"),
            P("section", "dp", "tensor"),
        ),
        check_vma=False,
    )
```
